16 devices in a mesh: dp: 4 (over y, z, core), sp: 4 (over x).
Axes of the slice: x: 4, y: 2, z: 1, core: 2. Of those that a mesh axis runs over, the one named last changes fastest.
The devices are a block of a 4x4x8 slice.
Arguments:
- q: bfloat16 [128, 48, 128], P('dp'), parts along dimension 0
- k: bfloat16 [128, 8192, 4, 128], P('dp', 'sp'), parts along dimension 0
- v: bfloat16 [128, 8192, 4, 128], P('dp', 'sp'), parts along dimension 0
Outputs:
- q: bfloat16 [128, 48, 128], P('dp'), parts along dimension 0
There are 4 independent parts. The reference program is written for one: setup_inputs(seed, part) draws one part's arguments, and reference() takes and returns one part's arrays. A program takes and returns all parts, laid end to end along the dimension named above; each array names one.
All inputs are finite; a program needn't handle non-finite values.
Results may differ from the reference program's by a relative error of at most 0.012.
Values are sent between devices in bfloat16 or wider.
A program may use at most 768 MiB of HBM per device.

```python
import jax
import jax.numpy as jnp

BATCH = 32
CACHE = 8192
HEADS = 48
KV_HEADS = 4
HEAD = 128


def setup_inputs(seed: int = 0, part: int = 0) -> dict:
    kq, kk, kv = (jax.random.fold_in(k, part) for k in jax.random.split(jax.random.key(seed), 3))
    return {
        "q": (3 * jax.random.normal(kq, (BATCH, HEADS, HEAD), jnp.float32)).astype(jnp.bfloat16),
        "k": jax.random.normal(kk, (BATCH, CACHE, KV_HEADS, HEAD), jnp.float32).astype(jnp.bfloat16),
        "v": jax.random.normal(kv, (BATCH, CACHE, KV_HEADS, HEAD), jnp.float32).astype(jnp.bfloat16),
    }


def einsum(form, a, b):
    return jnp.einsum(form, a.astype(jnp.float32), b.astype(jnp.float32))


def reference(q, k, v):
    grouped = q.reshape(BATCH, KV_HEADS, -1, HEAD)
    scores = einsum("bgsd,bugd->bgsu", grouped, k) * HEAD**-0.5
    weights = jax.nn.softmax(scores, -1).astype(jnp.bfloat16)
    return einsum("bgsu,bugd->bgsd", weights, v).astype(jnp.bfloat16).reshape(BATCH, HEADS, HEAD)
```

```python
import functools
import math

import jax
import jax.numpy as jnp
from jax import lax
from jax.experimental import pallas as pl
from jax.experimental.pallas import tpu as pltpu
from jax.sharding import PartitionSpec as P

MESH = pl.DeviceIdType.MESH
F32, BF16 = jnp.float32, jnp.bfloat16
SLOTS = 6
LAG = 4
TILE = 256


def lane_fold(x, op):
    for shift in (4, 8, 16, 32, 64):
        x = op(x, pltpu.roll(x, shift, 1))
    return x


def kernel(n, heads_kv, q_hbm, k_hbm, v_hbm, out_ref, qbuf, kbuf, vbuf, s0, s1, h0, h1, m0, m1, l0, l1, mask_ref, part, stat, qsem, ksem, vsem,
           part_send, part_recv, stat_send, stat_recv):
    me = lax.axis_index("sp")
    batch, heads, head = qbuf.shape
    slots, rows = kbuf.shape[:2]
    half = rows // 2
    tiles = half // TILE
    factor = head**-0.5 * math.log2(math.e)
    groups = batch // 2 - 1

    def k_copy(i):
        slot = lax.rem(i, slots)
        return pltpu.make_async_copy(k_hbm.at[i], kbuf.at[slot], ksem.at[slot])

    def v_copy(i):
        slot = lax.rem(i, slots)
        return pltpu.make_async_copy(v_hbm.at[i], vbuf.at[slot], vsem.at[slot])

    def transfers(g, first, count):
        out = []
        for off in (1, n - 1, *range(2, n - 1)):
            to = {"sp": lax.rem(me + off, n)}
            for buf, ssem, rsem in ((part, part_send, part_recv), (stat, stat_send, stat_recv)):
                ref = buf.at[me, pl.ds(first, count)]
                out.append(pltpu.make_async_remote_copy(ref, ref, ssem.at[g, off - 1], rsem.at[g, off - 1], device_id=to, device_id_type=MESH))
        return out

    def arrivals(g, first, count):
        out = []
        for off in range(1, n):
            src = lax.rem(me + n - off, n)
            for buf, ssem, rsem in ((part, part_send, part_recv), (stat, stat_send, stat_recv)):
                ref = buf.at[src, pl.ds(first, count)]
                out.append(pltpu.make_async_remote_copy(ref, ref, ssem.at[g, off - 1], rsem.at[g, off - 1], device_id={"sp": src}, device_id_type=MESH))
        return out

    q_copy = pltpu.make_async_copy(q_hbm, qbuf, qsem)
    q_copy.start()
    for i in range(slots - 1):
        k_copy(i).start()
        if i < slots - 2:
            v_copy(i).start()

    barrier = pltpu.get_barrier_semaphore()
    for off in range(1, n):
        pl.semaphore_signal(barrier, inc=1, device_id={"sp": lax.rem(me + off, n)}, device_id_type=MESH)

    per = heads // heads_kv
    own = lax.broadcasted_iota(jnp.int32, (heads, TILE), 0) // per == lax.rem(lax.broadcasted_iota(jnp.int32, (heads, TILE), 1), heads_kv)
    mask_ref[...] = jnp.where(own, 1.0, 0.0).astype(BF16)
    kind = lax.rem(lax.broadcasted_iota(jnp.int32, (8, TILE), 1), heads_kv)
    lane = lax.broadcasted_iota(jnp.int32, (8, 128), 1)
    low = lax.broadcasted_iota(jnp.int32, (8, 128), 0) < 4

    def scores(i, s_ref, h_ref):
        slot = lax.rem(i, slots)
        q = qbuf[i]
        zero = jnp.zeros_like(q)
        lhs = jnp.concatenate([jnp.concatenate([q, zero], 1), jnp.concatenate([zero, q], 1)], 0)
        top = None
        for c in range(tiles):
            lanes = slice(c * TILE, (c + 1) * TILE)
            rhs = jnp.concatenate([kbuf[slot, c * TILE : (c + 1) * TILE, :], kbuf[slot, half + c * TILE : half + (c + 1) * TILE, :]], 1)
            s = lax.dot_general(lhs, rhs, (((1,), (1,)), ((), ())), preferred_element_type=F32)
            for x in range(2):
                r = s[heads * x : heads * (x + 1)]
                a = jnp.where(kind == 0, r[0:8], jnp.where(kind == 1, r[16:24], jnp.where(kind == 2, r[24:32], r[40:48])))
                b = jnp.where(kind < 2, r[8:16], r[32:40])
                s_ref[x, 0:8, lanes] = a
                s_ref[x, 8:16, lanes] = b
                top = (a, b) if top is None else (jnp.maximum(top[0], a), jnp.maximum(top[1], b))
            if c % 2:
                yield
        for x in range(2):
            h_ref[x] = jnp.maximum(top[x][:, :128], top[x][:, 128:])

    def weigh(i, s_ref, h_ref, m_ref, l_ref):
        slot = lax.rem(i, slots)
        high = [lane_fold(h_ref[x], jnp.maximum) for x in range(2)]
        for x in range(2):
            m_ref[x] = high[x]
        yield
        wide = [jnp.concatenate([h, h], 1) for h in high]
        sums = [jnp.zeros((8, TILE), F32), jnp.zeros((8, TILE), F32)]
        acc = [None, None]
        mask = mask_ref[...]
        for c in range(tiles):
            lanes = slice(c * TILE, (c + 1) * TILE)
            both = []
            for x in range(2):
                a = jnp.exp2((s_ref[x, 0:8, lanes] - wide[0]) * factor)
                b = jnp.exp2((s_ref[x, 8:16, lanes] - wide[1]) * factor)
                sums = [sums[0] + a, sums[1] + b]
                both.append(jnp.concatenate([a, b, a, a, b, a], 0).astype(BF16) * mask)
            w = jnp.concatenate(both, 0)
            rhs = jnp.concatenate([vbuf[slot, c * TILE : (c + 1) * TILE, :], vbuf[slot, half + c * TILE : half + (c + 1) * TILE, :]], 1)
            o = jnp.dot(w, rhs, preferred_element_type=F32)
            acc[c % 2] = o if acc[c % 2] is None else acc[c % 2] + o
            if c % 2:
                yield
        o = acc[0] + acc[1]
        part[me, i] = (o[:heads, :head] + o[heads:, head:]).astype(BF16)
        for x in range(2):
            l_ref[x] = sums[x][:, :128] + sums[x][:, 128:]

    def settle(i, m_ref, l_ref):
        sums = [lane_fold(l_ref[x], jnp.add) for x in range(2)]
        stat[me, i] = jnp.where(lane < 32, m_ref[0], jnp.where(lane < 64, m_ref[1], jnp.where(lane < 96, sums[0], sums[1])))
        yield

    def run(*gens):
        gens = list(gens)
        while gens:
            for g in list(gens):
                try:
                    next(g)
                except StopIteration:
                    gens.remove(g)

    def combine(i):
        st = [stat[p, i] for p in range(n)]
        top = functools.reduce(jnp.maximum, st)
        scale = [jnp.exp2((s - top) * factor) for s in st]
        total = sum(w * pltpu.roll(s, 64, 1) for w, s in zip(scale, st))
        inv = 1.0 / total
        yield
        acc = None
        for p in range(n):
            w = scale[p] * inv

            def col(c):
                return jnp.broadcast_to(w[:, c : c + 1], (8, head))

            m01 = jnp.where(low, col(32), col(33))
            m23 = jnp.where(low, col(34), col(35))
            full = jnp.concatenate([col(0), m01, col(1), col(2), m23, col(3)], 0)
            term = part[p, i].astype(F32) * full
            acc = term if acc is None else acc + term
            yield
        out_ref[i] = acc.astype(BF16)

    def wait_arrivals(g, first, count):
        for c in arrivals(g, first, count):
            c.wait_recv()

    def send(g, first, count):
        for c in transfers(g, first, count):
            c.start()

    def wait_sent(g, first, count):
        for c in transfers(g, first, count):
            c.wait_send()

    q_copy.wait()
    k_copy(0).wait()
    run(scores(0, s0, h0))
    pl.semaphore_wait(barrier, n - 1)

    def body(full, j, _):
        for copy, i in ((k_copy, 2 * j - 1 + slots), (v_copy, 2 * j - 2 + slots), (k_copy, 2 * j + slots), (v_copy, 2 * j - 1 + slots)):
            @pl.when(i < batch)
            def _():
                copy(i).start()

        extra = []
        if full:
            wait_arrivals(j - LAG, 2 * (j - LAG), 2)
            wait_sent(j - LAG, 2 * (j - LAG), 2)
            send(j - 2, 2 * (j - 2), 2)
            extra = [combine(2 * (j - LAG)), combine(2 * (j - LAG) + 1)]
        else:
            @pl.when(j >= 2)
            def _():
                send(j - 2, 2 * (j - 2), 2)

        k_copy(2 * j + 1).wait()
        v_copy(2 * j).wait()
        k_copy(2 * j + 2).wait()
        v_copy(2 * j + 1).wait()
        run(scores(2 * j + 1, s1, h1), weigh(2 * j, s0, h0, m0, l0), settle(lax.max(2 * j - 1, 0), m1, l1), *extra[:1])
        run(scores(2 * j + 2, s0, h0), weigh(2 * j + 1, s1, h1, m1, l1), settle(2 * j, m0, l0), *extra[1:])
        return 0

    lax.fori_loop(0, LAG, functools.partial(body, False), 0)
    lax.fori_loop(LAG, groups, functools.partial(body, True), 0)
    last = batch - 1
    before = (groups - 2, 2 * (groups - 2), 2)
    sent = [(groups - 1, 2 * (groups - 1), 2), (groups, last - 1, 1), (groups + 1, last, 1)]
    send(*before)
    k_copy(last).wait()
    v_copy(last - 1).wait()
    run(scores(last, s1, h1), weigh(last - 1, s0, h0, m0, l0), settle(last - 2, m1, l1))
    send(*sent[0])
    run(settle(last - 1, m0, l0))
    send(*sent[1])
    v_copy(last).wait()
    run(weigh(last, s1, h1, m1, l1))
    run(settle(last, m1, l1))
    send(*sent[2])

    def rest(g, _):
        wait_arrivals(g, 2 * g, 2)
        wait_sent(g, 2 * g, 2)
        run(combine(2 * g), combine(2 * g + 1))
        return 0

    lax.fori_loop(groups - LAG, groups, rest, 0)
    for s in sent[1:]:
        wait_arrivals(*s)
        run(combine(s[1]))
    for s in sent[1:]:
        wait_sent(*s)


def solution(mesh):
    n = mesh.shape["sp"]

    def step(q, k, v):
        batch, heads, head = q.shape
        tokens, heads_kv = k.shape[1:3]
        rows = tokens * heads_kv
        groups = batch // 2 + 1
        any_spec = pl.BlockSpec(memory_space=pl.ANY)
        return pl.pallas_call(
            functools.partial(kernel, n, heads_kv),
            out_shape=jax.ShapeDtypeStruct(q.shape, BF16),
            in_specs=[any_spec] * 3,
            out_specs=pl.BlockSpec(memory_space=pltpu.VMEM),
            scratch_shapes=[
                pltpu.VMEM((batch, heads, head), BF16),
                pltpu.VMEM((SLOTS, rows, head), BF16),
                pltpu.VMEM((SLOTS, rows, head), BF16),
                pltpu.VMEM((2, 16, rows // 2), F32),
                pltpu.VMEM((2, 16, rows // 2), F32),
                *[pltpu.VMEM((2, 8, 128), F32)] * 6,
                pltpu.VMEM((heads, TILE), BF16),
                pltpu.VMEM((n, batch, heads, head), BF16),
                pltpu.VMEM((n, batch, 8, 128), F32),
                pltpu.SemaphoreType.DMA,
                pltpu.SemaphoreType.DMA((SLOTS,)),
                pltpu.SemaphoreType.DMA((SLOTS,)),
                pltpu.SemaphoreType.DMA((groups, n - 1)),
                pltpu.SemaphoreType.DMA((groups, n - 1)),
                pltpu.SemaphoreType.DMA((groups, n - 1)),
                pltpu.SemaphoreType.DMA((groups, n - 1)),
            ],
            compiler_params=pltpu.CompilerParams(collective_id=0, has_side_effects=True, vmem_limit_bytes=60 * 2**20),
        )(q, k.reshape(batch, rows, head), v.reshape(batch, rows, head))

    return jax.shard_map(
        step,
        mesh=mesh,
        in_specs=(P("dp", None, None), P("dp", "sp", None, None), P("dp", "sp", None, None)),
        out_specs=P("dp", None, None),
        check_vma=False,
    )
```

```python
import functools
import math

import jax
import jax.numpy as jnp
from jax import lax
from jax.experimental import pallas as pl
from jax.experimental.pallas import tpu as pltpu
from jax.sharding import PartitionSpec as P

MESH = pl.DeviceIdType.MESH
F32, BF16 = jnp.float32, jnp.bfloat16
SLOTS = 6
LAG = 4
LEAD = 4
TILE = 256


def lane_fold(x, kind, kinds, reduce, fill):
    out = None
    for g in range(kinds):
        r = reduce(jnp.where(kind == g, x, fill), axis=1, keepdims=True)
        out = jnp.broadcast_to(r, x.shape) if out is None else jnp.where(kind == g, r, out)
    return out


def kernel(n, heads_kv, q_hbm, k_hbm, v_hbm, out_ref, qbuf, kbuf, vbuf, s0, s1, h0, h1, m0, m1, l0, l1, mask_ref, part, stat, qsem, ksem, vsem,
           part_send, part_recv, stat_send, stat_recv):
    me = lax.axis_index("sp")
    batch, heads, head = qbuf.shape
    slots, rows = kbuf.shape[:2]
    half = rows // 2
    tiles = half // TILE
    factor = head**-0.5 * math.log2(math.e)
    groups = batch // 2 - 1

    def k_copy(i):
        slot = lax.rem(i, slots)
        return pltpu.make_async_copy(k_hbm.at[i], kbuf.at[slot], ksem.at[slot])

    def v_copy(i):
        slot = lax.rem(i, slots)
        return pltpu.make_async_copy(v_hbm.at[i], vbuf.at[slot], vsem.at[slot])

    def transfers(g, first, count):
        out = []
        for off in (1, n - 1, *range(2, n - 1)):
            to = {"sp": lax.rem(me + off, n)}
            for buf, ssem, rsem in ((part, part_send, part_recv), (stat, stat_send, stat_recv)):
                ref = buf.at[me, pl.ds(first, count)]
                out.append(pltpu.make_async_remote_copy(ref, ref, ssem.at[g, off - 1], rsem.at[g, off - 1], device_id=to, device_id_type=MESH))
        return out

    def arrivals(g, first, count):
        out = []
        for off in range(1, n):
            src = lax.rem(me + n - off, n)
            for buf, ssem, rsem in ((part, part_send, part_recv), (stat, stat_send, stat_recv)):
                ref = buf.at[src, pl.ds(first, count)]
                out.append(pltpu.make_async_remote_copy(ref, ref, ssem.at[g, off - 1], rsem.at[g, off - 1], device_id={"sp": src}, device_id_type=MESH))
        return out

    q_copy = pltpu.make_async_copy(q_hbm, qbuf, qsem)
    q_copy.start()
    k_copy(0).start()
    for i in range(1, slots):
        k_copy(i).start()
        v_copy(i - 1).start()

    barrier = pltpu.get_barrier_semaphore()
    for off in range(1, n):
        pl.semaphore_signal(barrier, inc=1, device_id={"sp": lax.rem(me + off, n)}, device_id_type=MESH)

    per = heads // heads_kv
    own = lax.broadcasted_iota(jnp.int32, (heads, TILE), 0) // per == lax.rem(lax.broadcasted_iota(jnp.int32, (heads, TILE), 1), heads_kv)
    mask_ref[...] = jnp.where(own, 1.0, 0.0).astype(BF16)
    kind = lax.rem(lax.broadcasted_iota(jnp.int32, (8, TILE), 1), heads_kv)
    lane = lax.broadcasted_iota(jnp.int32, (8, 128), 1)
    low = lax.broadcasted_iota(jnp.int32, (8, 128), 0) < 4

    def scores(i, s_ref, h_ref):
        slot = lax.rem(i, slots)
        q = qbuf[i]
        zero = jnp.zeros_like(q)
        lhs = jnp.concatenate([jnp.concatenate([q, zero], 1), jnp.concatenate([zero, q], 1)], 0)
        top = None
        for c in range(tiles):
            lanes = slice(c * TILE, (c + 1) * TILE)
            rhs = jnp.concatenate([kbuf[slot, c * TILE : (c + 1) * TILE, :], kbuf[slot, half + c * TILE : half + (c + 1) * TILE, :]], 1)
            s = lax.dot_general(lhs, rhs, (((1,), (1,)), ((), ())), preferred_element_type=F32)
            for x in range(2):
                r = s[heads * x : heads * (x + 1)]
                a = jnp.where(kind == 0, r[0:8], jnp.where(kind == 1, r[16:24], jnp.where(kind == 2, r[24:32], r[40:48])))
                b = jnp.where(kind < 2, r[8:16], r[32:40])
                s_ref[x, 0:8, lanes] = a
                s_ref[x, 8:16, lanes] = b
                top = (a, b) if top is None else (jnp.maximum(top[0], a), jnp.maximum(top[1], b))
            if c % 2:
                yield
        for x in range(2):
            h_ref[x] = jnp.maximum(top[x][:, :128], top[x][:, 128:])

    def weigh(i, s_ref, h_ref, m_ref, l_ref):
        slot = lax.rem(i, slots)
        high = [lane_fold(h_ref[x], kind[:, :128], heads_kv, jnp.max, -jnp.inf) for x in range(2)]
        for x in range(2):
            m_ref[x] = high[x]
        yield
        wide = [jnp.concatenate([h, h], 1) for h in high]
        sums = [jnp.zeros((8, TILE), F32), jnp.zeros((8, TILE), F32)]
        acc = [None, None]
        mask = mask_ref[...]
        for c in range(tiles):
            lanes = slice(c * TILE, (c + 1) * TILE)
            both = []
            for x in range(2):
                a = jnp.exp2((s_ref[x, 0:8, lanes] - wide[0]) * factor)
                b = jnp.exp2((s_ref[x, 8:16, lanes] - wide[1]) * factor)
                sums = [sums[0] + a, sums[1] + b]
                both.append(jnp.concatenate([a, b, a, a, b, a], 0).astype(BF16) * mask)
            w = jnp.concatenate(both, 0)
            rhs = jnp.concatenate([vbuf[slot, c * TILE : (c + 1) * TILE, :], vbuf[slot, half + c * TILE : half + (c + 1) * TILE, :]], 1)
            o = jnp.dot(w, rhs, preferred_element_type=F32)
            acc[c % 2] = o if acc[c % 2] is None else acc[c % 2] + o
            if c % 2:
                yield
        o = acc[0] + acc[1]
        part[me, i] = (o[:heads, :head] + o[heads:, head:]).astype(BF16)
        for x in range(2):
            l_ref[x] = sums[x][:, :128] + sums[x][:, 128:]

    def settle(i, m_ref, l_ref):
        sums = [lane_fold(l_ref[x], kind[:, :128], heads_kv, jnp.sum, 0.0) for x in range(2)]
        stat[me, i] = jnp.where(lane < 32, m_ref[0], jnp.where(lane < 64, m_ref[1], jnp.where(lane < 96, sums[0], sums[1])))
        yield

    def run(*gens):
        gens = list(gens)
        while gens:
            for g in list(gens):
                try:
                    next(g)
                except StopIteration:
                    gens.remove(g)

    def block(first, second, *others):
        others = list(others)

        def step(g, count=1):
            for _ in range(count):
                next(g, None)

        step(second)
        step(first, LEAD)
        while True:
            for g in others:
                step(g)
            step(second, 2)
            if next(first, StopIteration) is StopIteration:
                break
        run(second, *others)

    def combine(i):
        st = [stat[p, i] for p in range(n)]
        top = functools.reduce(jnp.maximum, st)
        scale = [jnp.exp2((s - top) * factor) for s in st]
        total = sum(w * pltpu.roll(s, 64, 1) for w, s in zip(scale, st))
        inv = 1.0 / total
        yield
        acc = None
        for p in range(n):
            w = scale[p] * inv

            def col(c):
                return jnp.broadcast_to(w[:, c : c + 1], (8, head))

            m01 = jnp.where(low, col(32), col(33))
            m23 = jnp.where(low, col(34), col(35))
            full = jnp.concatenate([col(0), m01, col(1), col(2), m23, col(3)], 0)
            term = part[p, i].astype(F32) * full
            acc = term if acc is None else acc + term
            yield
        out_ref[i] = acc.astype(BF16)

    def wait_arrivals(g, first, count):
        for c in arrivals(g, first, count):
            c.wait_recv()

    def send(g, first, count):
        for c in transfers(g, first, count):
            c.start()

    def wait_sent(g, first, count):
        for c in transfers(g, first, count):
            c.wait_send()

    q_copy.wait()
    k_copy(0).wait()
    run(scores(0, s0, h0))
    pl.semaphore_wait(barrier, n - 1)

    def fetch(i):
        for copy, later in ((k_copy, i + slots), (v_copy, i + slots - 1)):
            @pl.when(later < batch)
            def _():
                copy(later).start()

    def body(full, j, _):
        i = 2 * j
        fetch(i)
        extra = []
        if full:
            wait_arrivals(j - LAG, 2 * (j - LAG), 2)
            wait_sent(j - LAG, 2 * (j - LAG), 2)
            send(j - 2, 2 * (j - 2), 2)
            extra = [combine(2 * (j - LAG)), combine(2 * (j - LAG) + 1)]
        else:
            @pl.when(j >= 2)
            def _():
                send(j - 2, 2 * (j - 2), 2)

        k_copy(i + 1).wait()
        v_copy(i).wait()
        block(scores(i + 1, s1, h1), weigh(i, s0, h0, m0, l0), settle(lax.max(i - 1, 0), m1, l1), *extra[:1])
        fetch(i + 1)
        k_copy(i + 2).wait()
        v_copy(i + 1).wait()
        block(scores(i + 2, s0, h0), weigh(i + 1, s1, h1, m1, l1), settle(i, m0, l0), *extra[1:])
        return 0

    lax.fori_loop(0, LAG, functools.partial(body, False), 0)
    lax.fori_loop(LAG, groups, functools.partial(body, True), 0)
    last = batch - 1
    before = (groups - 2, 2 * (groups - 2), 2)
    sent = [(groups - 1, 2 * (groups - 1), 2), (groups, last - 1, 1), (groups + 1, last, 1)]
    k_copy(last).wait()
    run(scores(last, s1, h1), settle(last - 2, m1, l1))
    send(*before)
    send(*sent[0])
    v_copy(last - 1).wait()
    run(weigh(last - 1, s0, h0, m0, l0))
    run(settle(last - 1, m0, l0))
    send(*sent[1])
    v_copy(last).wait()
    run(weigh(last, s1, h1, m1, l1))
    run(settle(last, m1, l1))
    send(*sent[2])

    def rest(g, _):
        wait_arrivals(g, 2 * g, 2)
        wait_sent(g, 2 * g, 2)
        run(combine(2 * g), combine(2 * g + 1))
        return 0

    lax.fori_loop(groups - LAG, groups, rest, 0)
    for s in sent[1:]:
        wait_arrivals(*s)
        run(combine(s[1]))
    for s in sent[1:]:
        wait_sent(*s)


def solution(mesh):
    n = mesh.shape["sp"]

    def step(q, k, v):
        batch, heads, head = q.shape
        tokens, heads_kv = k.shape[1:3]
        rows = tokens * heads_kv
        groups = batch // 2 + 1
        any_spec = pl.BlockSpec(memory_space=pl.ANY)
        return pl.pallas_call(
            functools.partial(kernel, n, heads_kv),
            out_shape=pltpu.VMEM(q.shape, BF16),
            in_specs=[any_spec] * 3,
            out_specs=pl.BlockSpec(memory_space=pltpu.VMEM),
            scratch_shapes=[
                pltpu.VMEM((batch, heads, head), BF16),
                pltpu.VMEM((SLOTS, rows, head), BF16),
                pltpu.VMEM((SLOTS, rows, head), BF16),
                pltpu.VMEM((2, 16, rows // 2), F32),
                pltpu.VMEM((2, 16, rows // 2), F32),
                *[pltpu.VMEM((2, 8, 128), F32)] * 6,
                pltpu.VMEM((heads, TILE), BF16),
                pltpu.VMEM((n, batch, heads, head), BF16),
                pltpu.VMEM((n, batch, 8, 128), F32),
                pltpu.SemaphoreType.DMA,
                pltpu.SemaphoreType.DMA((SLOTS,)),
                pltpu.SemaphoreType.DMA((SLOTS,)),
                pltpu.SemaphoreType.DMA((groups, n - 1)),
                pltpu.SemaphoreType.DMA((groups, n - 1)),
                pltpu.SemaphoreType.DMA((groups, n - 1)),
                pltpu.SemaphoreType.DMA((groups, n - 1)),
            ],
            compiler_params=pltpu.CompilerParams(collective_id=0, has_side_effects=True, vmem_limit_bytes=48 * 2**20),
        )(pltpu.with_memory_space_constraint(q, pltpu.HBM), k.reshape(batch, rows, head), v.reshape(batch, rows, head))

    return jax.shard_map(
        step,
        mesh=mesh,
        in_specs=(P("dp", None, None), P("dp", "sp", None, None), P("dp", "sp", None, None)),
        out_specs=P("dp", None, None),
        check_vma=False,
    )
```

```python
import functools
import math

import jax
import jax.numpy as jnp
from jax import lax
from jax.experimental import pallas as pl
from jax.experimental.pallas import tpu as pltpu
from jax.sharding import PartitionSpec as P

MESH = pl.DeviceIdType.MESH
F32, BF16 = jnp.float32, jnp.bfloat16
SLOTS = 8
UNROLL = 4
LAG = 3
LEAD = 4
TILE = 256


def lane_fold(x, kind, kinds, reduce, fill):
    out = None
    for g in range(kinds):
        r = reduce(jnp.where(kind == g, x, fill), axis=1, keepdims=True)
        out = jnp.broadcast_to(r, x.shape) if out is None else jnp.where(kind == g, r, out)
    return out


def kernel(n, heads_kv, q_hbm, k_hbm, v_hbm, out_ref, qbuf, kbuf, vbuf, s0, s1, s2, h0, h1, h2, m0, m1, l0, l1, one_ref, mask_ref, part, stat, qsem, ksem, vsem,
           part_send, part_recv, stat_send, stat_recv):
    me = lax.axis_index("sp")
    batch, heads, head = qbuf.shape
    slots, rows = kbuf.shape[:2]
    half = rows // 2
    tiles = half // TILE
    factor = head**-0.5 * math.log2(math.e)
    groups = batch // UNROLL - 1
    last = batch - 1

    def k_copy(i):
        slot = lax.rem(i, slots)
        return pltpu.make_async_copy(k_hbm.at[i], kbuf.at[slot], ksem.at[slot])

    def v_copy(i):
        slot = lax.rem(i, slots)
        return pltpu.make_async_copy(v_hbm.at[i], vbuf.at[slot], vsem.at[slot])

    def transfers(g, first, count):
        out = []
        for off in (1, n - 1, *range(2, n - 1)):
            to = {"sp": lax.rem(me + off, n)}
            for buf, ssem, rsem in ((part, part_send, part_recv), (stat, stat_send, stat_recv)):
                ref = buf.at[me, pl.ds(first, count)]
                out.append(pltpu.make_async_remote_copy(ref, ref, ssem.at[g, off - 1], rsem.at[g, off - 1], device_id=to, device_id_type=MESH))
        return out

    def arrivals(g, first, count):
        out = []
        for off in range(1, n):
            src = lax.rem(me + n - off, n)
            for buf, ssem, rsem in ((part, part_send, part_recv), (stat, stat_send, stat_recv)):
                ref = buf.at[src, pl.ds(first, count)]
                out.append(pltpu.make_async_remote_copy(ref, ref, ssem.at[g, off - 1], rsem.at[g, off - 1], device_id={"sp": src}, device_id_type=MESH))
        return out

    q_copy = pltpu.make_async_copy(q_hbm, qbuf, qsem)
    q_copy.start()
    k_copy(0).start()
    for i in range(1, slots):
        k_copy(i).start()
        if i < slots - 1:
            v_copy(i - 1).start()

    barrier = pltpu.get_barrier_semaphore()
    for off in range(1, n):
        pl.semaphore_signal(barrier, inc=1, device_id={"sp": lax.rem(me + off, n)}, device_id_type=MESH)

    per = heads // heads_kv
    own = lax.broadcasted_iota(jnp.int32, (heads, TILE), 0) // per == lax.rem(lax.broadcasted_iota(jnp.int32, (heads, TILE), 1), heads_kv)
    one_ref[...] = jnp.ones_like(one_ref)
    mask_ref[...] = jnp.where(own, 1.0, 0.0).astype(BF16)
    kind = lax.rem(lax.broadcasted_iota(jnp.int32, (8, TILE), 1), heads_kv)
    lane = lax.broadcasted_iota(jnp.int32, (8, 128), 1)
    low = lax.broadcasted_iota(jnp.int32, (8, 128), 0) < 4

    def scores(i, s_ref, h_ref):
        slot = lax.rem(i, slots)
        q = qbuf[i]
        zero = jnp.zeros_like(q)
        lhs = jnp.concatenate([jnp.concatenate([q, zero], 1), jnp.concatenate([zero, q], 1)], 0)
        top = None
        for c in range(tiles):
            lanes = slice(c * TILE, (c + 1) * TILE)
            rhs = jnp.concatenate([kbuf[slot, c * TILE : (c + 1) * TILE, :], kbuf[slot, half + c * TILE : half + (c + 1) * TILE, :]], 1)
            s = lax.dot_general(lhs, rhs, (((1,), (1,)), ((), ())), preferred_element_type=F32)
            for x in range(2):
                r = s[heads * x : heads * (x + 1)]
                a = jnp.where(kind == 0, r[0:8], jnp.where(kind == 1, r[16:24], jnp.where(kind == 2, r[24:32], r[40:48])))
                b = jnp.where(kind < 2, r[8:16], r[32:40])
                s_ref[x, 0:8, lanes] = a
                s_ref[x, 8:16, lanes] = b
                top = (a, b) if top is None else (jnp.maximum(top[0], a), jnp.maximum(top[1], b))
            if c % 2:
                yield
        for x in range(2):
            h_ref[x] = jnp.maximum(top[x][:, :128], top[x][:, 128:])

    def weigh(i, s_ref, h_ref, m_ref, l_ref, alone=False):
        slot = lax.rem(i, slots)
        high = [lane_fold(h_ref[x], kind[:, :128], heads_kv, jnp.max, -jnp.inf) for x in range(2)]
        for x in range(2):
            m_ref[x] = high[x]
        yield
        wide = [jnp.concatenate([h, h], 1) for h in high]
        sums = [jnp.zeros((8, TILE), F32), jnp.zeros((8, TILE), F32)]
        acc = [None, None]
        mask = mask_ref[...]
        for c in range(tiles):
            lanes = slice(c * TILE, (c + 1) * TILE)
            both = []
            for x in range(2):
                a = jnp.exp2((s_ref[x, 0:8, lanes] - wide[0]) * factor)
                b = jnp.exp2((s_ref[x, 8:16, lanes] - wide[1]) * factor)
                sums = [sums[0] + a, sums[1] + b]
                both.append(jnp.concatenate([a, b, a, a, b, a], 0).astype(BF16) * mask)
            w = jnp.concatenate(both, 0)
            rhs = jnp.concatenate([vbuf[slot, c * TILE : (c + 1) * TILE, :], vbuf[slot, half + c * TILE : half + (c + 1) * TILE, :]], 1)
            o = jnp.dot(w, rhs, preferred_element_type=F32)
            acc[c % 2] = o if acc[c % 2] is None else acc[c % 2] + o
            if c % 2:
                yield
        o = acc[0] + (acc[1] * one_ref[...] if alone else acc[1])
        part[me, i] = (o[:heads, :head] + o[heads:, head:]).astype(BF16)
        for x in range(2):
            l_ref[x] = sums[x][:, :128] + sums[x][:, 128:]

    def settle(i, m_ref, l_ref):
        sums = [lane_fold(l_ref[x], kind[:, :128], heads_kv, jnp.sum, 0.0) for x in range(2)]
        stat[me, i] = jnp.where(lane < 32, m_ref[0], jnp.where(lane < 64, m_ref[1], jnp.where(lane < 96, sums[0], sums[1])))
        yield

    def run(*gens):
        gens = list(gens)
        while gens:
            for g in list(gens):
                try:
                    next(g)
                except StopIteration:
                    gens.remove(g)

    def block(first, second, *others):
        others = list(others)

        def step(g, count=1):
            for _ in range(count):
                next(g, None)

        step(second)
        step(first, LEAD)
        while True:
            for g in others:
                step(g)
            step(second, 2)
            if next(first, StopIteration) is StopIteration:
                break
        run(second, *others)

    def combine(i):
        st = [stat[p, i] for p in range(n)]
        top = functools.reduce(jnp.maximum, st)
        scale = [jnp.exp2((s - top) * factor) for s in st]
        total = sum(w * pltpu.roll(s, 64, 1) for w, s in zip(scale, st))
        inv = 1.0 / total
        yield
        acc = None
        for p in range(n):
            w = scale[p] * inv

            def col(c):
                return jnp.broadcast_to(w[:, c : c + 1], (8, head))

            m01 = jnp.where(low, col(32), col(33))
            m23 = jnp.where(low, col(34), col(35))
            full = jnp.concatenate([col(0), m01, col(1), col(2), m23, col(3)], 0)
            term = part[p, i].astype(F32) * full
            acc = term if acc is None else acc + term
            yield
        out_ref[i] = acc.astype(BF16)

    def wait_arrivals(g, first, count):
        for c in arrivals(g, first, count):
            c.wait_recv()

    def send(g, first, count):
        for c in transfers(g, first, count):
            c.start()

    def wait_sent(g, first, count):
        for c in transfers(g, first, count):
            c.wait_send()

    q_copy.wait()
    k_copy(0).wait()
    run(scores(0, s0, h0))
    pl.semaphore_wait(barrier, n - 1)

    sets = ((s0, h0, m0, l0), (s1, h1, m1, l1))

    def fetch(i):
        for copy, later in ((k_copy, i + slots), (v_copy, i + slots - 2)):
            @pl.when(later < batch)
            def _():
                copy(later).start()

    def body(full, j, _):
        first = UNROLL * j
        extra = [()] * UNROLL
        if full:
            g = j - LAG
            wait_arrivals(g, UNROLL * g, UNROLL)
            wait_sent(g, UNROLL * g, UNROLL)
            send(j - 2, UNROLL * (j - 2), UNROLL)
            extra = [(combine(UNROLL * g + u),) for u in range(UNROLL)]
        else:
            @pl.when(j >= 2)
            def _():
                send(j - 2, UNROLL * (j - 2), UNROLL)

        together = UNROLL if full else UNROLL // 2
        for u in range(UNROLL):
            i = first + u
            fetch(i)
            if u % together == 0:
                for w in range(together):
                    k_copy(i + w + 1).wait()
                    v_copy(i + w).wait()
            now, then = sets[u % 2], sets[(u + 1) % 2]
            block(scores(i + 1, *then[:2]), weigh(i, *now), settle(lax.max(i - 1, 0), *then[2:]), *extra[u])
        return 0

    def whole(g):
        return g, UNROLL * g, UNROLL

    lax.fori_loop(0, LAG, functools.partial(body, False), 0)
    lax.fori_loop(LAG, groups, functools.partial(body, True), 0)
    tail = [(groups, last - 3, 3), (groups + 1, last, 1)]
    send(*whole(groups - 2))
    wait_arrivals(*whole(groups - LAG))
    wait_sent(*whole(groups - LAG))
    k_copy(last - 2).wait()
    v_copy(last - 3).wait()
    old = [combine(UNROLL * (groups - LAG) + u) for u in range(UNROLL)]
    block(scores(last - 2, s1, h1), weigh(last - 3, s0, h0, m0, l0), settle(last - 4, m1, l1), *old[:2])
    send(*whole(groups - 1))
    k_copy(last - 1).wait()
    k_copy(last).wait()
    run(scores(last - 1, s0, h0), settle(last - 3, m0, l0), old[2])
    run(scores(last, s2, h2), old[3])
    v_copy(last - 2).wait()
    run(weigh(last - 2, s1, h1, m1, l1, True))
    v_copy(last - 1).wait()
    run(weigh(last - 1, s0, h0, m0, l0, True), settle(last - 2, m1, l1))
    run(settle(last - 1, m0, l0))
    send(*tail[0])
    final = weigh(last, s2, h2, m1, l1, True)
    next(final)
    v_copy(last).wait()
    run(final)
    run(settle(last, m1, l1))
    send(*tail[1])

    def rest(g, _):
        wait_arrivals(*whole(g))
        wait_sent(*whole(g))
        run(*[combine(UNROLL * g + u) for u in range(UNROLL)])
        return 0

    lax.fori_loop(groups - LAG + 1, groups, rest, 0)
    for s in tail:
        wait_arrivals(*s)
        run(*[combine(s[1] + u) for u in range(s[2])])
    for s in tail:
        wait_sent(*s)


def solution(mesh):
    n = mesh.shape["sp"]

    def step(q, k, v):
        batch, heads, head = q.shape
        tokens, heads_kv = k.shape[1:3]
        rows = tokens * heads_kv
        groups = batch // UNROLL + 1
        any_spec = pl.BlockSpec(memory_space=pl.ANY)
        return pl.pallas_call(
            functools.partial(kernel, n, heads_kv),
            out_shape=pltpu.VMEM(q.shape, BF16),
            in_specs=[any_spec] * 3,
            out_specs=pl.BlockSpec(memory_space=pltpu.VMEM),
            scratch_shapes=[
                pltpu.VMEM((batch, heads, head), BF16),
                pltpu.VMEM((SLOTS, rows, head), BF16),
                pltpu.VMEM((SLOTS, rows, head), BF16),
                *[pltpu.VMEM((2, 16, rows // 2), F32)] * 3,
                *[pltpu.VMEM((2, 8, 128), F32)] * 7,
                pltpu.VMEM((2 * heads, TILE), F32),
                pltpu.VMEM((heads, TILE), BF16),
                pltpu.VMEM((n, batch, heads, head), BF16),
                pltpu.VMEM((n, batch, 8, 128), F32),
                pltpu.SemaphoreType.DMA,
                pltpu.SemaphoreType.DMA((SLOTS,)),
                pltpu.SemaphoreType.DMA((SLOTS,)),
                pltpu.SemaphoreType.DMA((groups, n - 1)),
                pltpu.SemaphoreType.DMA((groups, n - 1)),
                pltpu.SemaphoreType.DMA((groups, n - 1)),
                pltpu.SemaphoreType.DMA((groups, n - 1)),
            ],
            compiler_params=pltpu.CompilerParams(collective_id=0, has_side_effects=True, vmem_limit_bytes=52 * 2**20),
        )(pltpu.with_memory_space_constraint(q, pltpu.HBM), k.reshape(batch, rows, head), v.reshape(batch, rows, head))

    return jax.shard_map(
        step,
        mesh=mesh,
        in_specs=(P("dp", None, None), P("dp", "sp", None, None), P("dp", "sp", None, None)),
        out_specs=P("dp", None, None),
        check_vma=False,
    )
```

```python
import functools
import math

import jax
import jax.numpy as jnp
from jax import lax
from jax.experimental import pallas as pl
from jax.experimental.pallas import tpu as pltpu
from jax.sharding import PartitionSpec as P

MESH = pl.DeviceIdType.MESH
F32, BF16 = jnp.float32, jnp.bfloat16
SLOTS = 4
LAG = 4
LEAD = 4
TILE = 256


def lane_fold(x, kind, kinds, reduce, fill):
    out = None
    for g in range(kinds):
        r = reduce(jnp.where(kind == g, x, fill), axis=1, keepdims=True)
        out = jnp.broadcast_to(r, x.shape) if out is None else jnp.where(kind == g, r, out)
    return out


def kernel(n, heads_kv, q_hbm, k_hbm, v_hbm, out_ref, qbuf, kbuf, vbuf, s0, s1, h0, h1, m0, m1, l0, l1, one_ref, mask_ref, part, stat, qsem, ksem, vsem,
           part_send, part_recv, stat_send, stat_recv):
    me = lax.axis_index("sp")
    batch, heads, head = qbuf.shape
    slots, rows = kbuf.shape[:2]
    half = rows // 2
    tiles = half // TILE
    factor = head**-0.5 * math.log2(math.e)
    groups = batch // 2 - 1

    def k_copy(i):
        slot = lax.rem(i, slots)
        return pltpu.make_async_copy(k_hbm.at[i], kbuf.at[slot], ksem.at[slot])

    def v_copy(i):
        slot = lax.rem(i, slots)
        return pltpu.make_async_copy(v_hbm.at[i], vbuf.at[slot], vsem.at[slot])

    def transfers(g, first, count):
        out = []
        for off in (1, n - 1, *range(2, n - 1)):
            to = {"sp": lax.rem(me + off, n)}
            for buf, ssem, rsem in ((part, part_send, part_recv), (stat, stat_send, stat_recv)):
                ref = buf.at[me, pl.ds(first, count)]
                out.append(pltpu.make_async_remote_copy(ref, ref, ssem.at[g, off - 1], rsem.at[g, off - 1], device_id=to, device_id_type=MESH))
        return out

    def arrivals(g, first, count):
        out = []
        for off in range(1, n):
            src = lax.rem(me + n - off, n)
            for buf, ssem, rsem in ((part, part_send, part_recv), (stat, stat_send, stat_recv)):
                ref = buf.at[src, pl.ds(first, count)]
                out.append(pltpu.make_async_remote_copy(ref, ref, ssem.at[g, off - 1], rsem.at[g, off - 1], device_id={"sp": src}, device_id_type=MESH))
        return out

    q_copy = pltpu.make_async_copy(q_hbm, qbuf, qsem)
    q_copy.start()
    k_copy(0).start()

    barrier = pltpu.get_barrier_semaphore()
    for off in range(1, n):
        pl.semaphore_signal(barrier, inc=1, device_id={"sp": lax.rem(me + off, n)}, device_id_type=MESH)

    per = heads // heads_kv
    own = lax.broadcasted_iota(jnp.int32, (heads, TILE), 0) // per == lax.rem(lax.broadcasted_iota(jnp.int32, (heads, TILE), 1), heads_kv)
    one_ref[...] = jnp.ones_like(one_ref)
    mask_ref[...] = jnp.where(own, 1.0, 0.0).astype(BF16)
    kind = lax.rem(lax.broadcasted_iota(jnp.int32, (8, TILE), 1), heads_kv)
    lane = lax.broadcasted_iota(jnp.int32, (8, 128), 1)
    low = lax.broadcasted_iota(jnp.int32, (8, 128), 0) < 4

    def scores(i, s_ref, h_ref):
        slot = lax.rem(i, slots)
        q = qbuf[i]
        zero = jnp.zeros_like(q)
        lhs = jnp.concatenate([jnp.concatenate([q, zero], 1), jnp.concatenate([zero, q], 1)], 0)
        top = None
        for c in range(tiles):
            lanes = slice(c * TILE, (c + 1) * TILE)
            rhs = jnp.concatenate([kbuf[slot, c * TILE : (c + 1) * TILE, :], kbuf[slot, half + c * TILE : half + (c + 1) * TILE, :]], 1)
            s = lax.dot_general(lhs, rhs, (((1,), (1,)), ((), ())), preferred_element_type=F32)
            for x in range(2):
                r = s[heads * x : heads * (x + 1)]
                a = jnp.where(kind == 0, r[0:8], jnp.where(kind == 1, r[16:24], jnp.where(kind == 2, r[24:32], r[40:48])))
                b = jnp.where(kind < 2, r[8:16], r[32:40])
                s_ref[x, 0:8, lanes] = a
                s_ref[x, 8:16, lanes] = b
                top = (a, b) if top is None else (jnp.maximum(top[0], a), jnp.maximum(top[1], b))
            if c % 2:
                yield
        for x in range(2):
            h_ref[x] = jnp.maximum(top[x][:, :128], top[x][:, 128:])

    def weigh(i, s_ref, h_ref, m_ref, l_ref, alone=False):
        slot = lax.rem(i, slots)
        high = [lane_fold(h_ref[x], kind[:, :128], heads_kv, jnp.max, -jnp.inf) for x in range(2)]
        for x in range(2):
            m_ref[x] = high[x]
        yield
        wide = [jnp.concatenate([h, h], 1) for h in high]
        sums = [jnp.zeros((8, TILE), F32), jnp.zeros((8, TILE), F32)]
        acc = [None, None]
        mask = mask_ref[...]
        for c in range(tiles):
            lanes = slice(c * TILE, (c + 1) * TILE)
            both = []
            for x in range(2):
                a = jnp.exp2((s_ref[x, 0:8, lanes] - wide[0]) * factor)
                b = jnp.exp2((s_ref[x, 8:16, lanes] - wide[1]) * factor)
                sums = [sums[0] + a, sums[1] + b]
                both.append(jnp.concatenate([a, b, a, a, b, a], 0).astype(BF16) * mask)
            w = jnp.concatenate(both, 0)
            rhs = jnp.concatenate([vbuf[slot, c * TILE : (c + 1) * TILE, :], vbuf[slot, half + c * TILE : half + (c + 1) * TILE, :]], 1)
            o = jnp.dot(w, rhs, preferred_element_type=F32)
            acc[c % 2] = o if acc[c % 2] is None else acc[c % 2] + o
            if c % 2:
                yield
        o = acc[0] + (acc[1] * one_ref[...] if alone else acc[1])
        part[me, i] = (o[:heads, :head] + o[heads:, head:]).astype(BF16)
        for x in range(2):
            l_ref[x] = sums[x][:, :128] + sums[x][:, 128:]

    def settle(i, m_ref, l_ref):
        sums = [lane_fold(l_ref[x], kind[:, :128], heads_kv, jnp.sum, 0.0) for x in range(2)]
        stat[me, i] = jnp.where(lane < 32, m_ref[0], jnp.where(lane < 64, m_ref[1], jnp.where(lane < 96, sums[0], sums[1])))
        yield

    def run(*gens):
        gens = list(gens)
        while gens:
            for g in list(gens):
                try:
                    next(g)
                except StopIteration:
                    gens.remove(g)

    def block(first, second, *others):
        others = list(others)

        def step(g, count=1):
            for _ in range(count):
                next(g, None)

        step(second)
        step(first, LEAD)
        while True:
            for g in others:
                step(g)
            step(second, 2)
            if next(first, StopIteration) is StopIteration:
                break
        run(second, *others)

    def combine(i):
        st = [stat[p, i] for p in range(n)]
        top = functools.reduce(jnp.maximum, st)
        scale = [jnp.exp2((s - top) * factor) for s in st]
        total = sum(w * pltpu.roll(s, 64, 1) for w, s in zip(scale, st))
        inv = 1.0 / total
        yield
        acc = None
        for p in range(n):
            w = scale[p] * inv

            def col(c):
                return jnp.broadcast_to(w[:, c : c + 1], (8, head))

            m01 = jnp.where(low, col(32), col(33))
            m23 = jnp.where(low, col(34), col(35))
            full = jnp.concatenate([col(0), m01, col(1), col(2), m23, col(3)], 0)
            term = part[p, i].astype(F32) * full
            acc = term if acc is None else acc + term
            yield
        out_ref[i] = acc.astype(BF16)

    def wait_arrivals(g, first, count):
        for c in arrivals(g, first, count):
            c.wait_recv()

    def send(g, first, count):
        for c in transfers(g, first, count):
            c.start()

    def wait_sent(g, first, count):
        for c in transfers(g, first, count):
            c.wait_send()

    def pair(i):
        k_copy(i).start()
        v_copy(i - 1).start()

    pair(1)
    q_copy.wait()
    k_copy(0).wait()
    pair(2)
    run(scores(0, s0, h0))
    pair(3)
    pl.semaphore_wait(barrier, n - 1)

    def fetch(i):
        for copy, later in ((k_copy, i + slots), (v_copy, i + slots - 1)):
            @pl.when(later < batch)
            def _():
                copy(later).start()

    def body(full, j, _):
        i = 2 * j
        fetch(i)
        extra = []
        if full:
            wait_arrivals(j - LAG, 2 * (j - LAG), 2)
            wait_sent(j - LAG, 2 * (j - LAG), 2)
            send(j - 2, 2 * (j - 2), 2)
            extra = [combine(2 * (j - LAG)), combine(2 * (j - LAG) + 1)]
        else:
            @pl.when(j >= 2)
            def _():
                send(j - 2, 2 * (j - 2), 2)

        k_copy(i + 1).wait()
        v_copy(i).wait()
        block(scores(i + 1, s1, h1), weigh(i, s0, h0, m0, l0), settle(lax.max(i - 1, 0), m1, l1), *extra[:1])
        fetch(i + 1)
        k_copy(i + 2).wait()
        v_copy(i + 1).wait()
        block(scores(i + 2, s0, h0), weigh(i + 1, s1, h1, m1, l1), settle(i, m0, l0), *extra[1:])
        return 0

    lax.fori_loop(0, LAG, functools.partial(body, False), 0)
    lax.fori_loop(LAG, groups, functools.partial(body, True), 0)
    last = batch - 1
    before = (groups - 2, 2 * (groups - 2), 2)
    sent = [(groups - 1, 2 * (groups - 1), 2), (groups, last - 1, 1), (groups + 1, last, 1)]
    k_copy(last).wait()
    run(scores(last, s1, h1), settle(last - 2, m1, l1))
    send(*before)
    send(*sent[0])
    v_copy(last - 1).wait()
    run(weigh(last - 1, s0, h0, m0, l0, True))
    run(settle(last - 1, m0, l0))
    send(*sent[1])
    v_copy(last).wait()
    run(weigh(last, s1, h1, m1, l1, True))
    run(settle(last, m1, l1))
    send(*sent[2])

    def rest(g, _):
        wait_arrivals(g, 2 * g, 2)
        wait_sent(g, 2 * g, 2)
        run(combine(2 * g), combine(2 * g + 1))
        return 0

    lax.fori_loop(groups - LAG, groups, rest, 0)
    for s in sent[1:]:
        wait_arrivals(*s)
        run(combine(s[1]))
    for s in sent[1:]:
        wait_sent(*s)


def solution(mesh):
    n = mesh.shape["sp"]

    def step(q, k, v):
        batch, heads, head = q.shape
        tokens, heads_kv = k.shape[1:3]
        rows = tokens * heads_kv
        groups = batch // 2 + 1
        any_spec = pl.BlockSpec(memory_space=pl.ANY)
        return pl.pallas_call(
            functools.partial(kernel, n, heads_kv),
            out_shape=pltpu.VMEM(q.shape, BF16),
            in_specs=[any_spec] * 3,
            out_specs=pl.BlockSpec(memory_space=pltpu.VMEM),
            scratch_shapes=[
                pltpu.VMEM((batch, heads, head), BF16),
                pltpu.VMEM((SLOTS, rows, head), BF16),
                pltpu.VMEM((SLOTS, rows, head), BF16),
                pltpu.VMEM((2, 16, rows // 2), F32),
                pltpu.VMEM((2, 16, rows // 2), F32),
                *[pltpu.VMEM((2, 8, 128), F32)] * 6,
                pltpu.VMEM((2 * heads, TILE), F32),
                pltpu.VMEM((heads, TILE), BF16),
                pltpu.VMEM((n, batch, heads, head), BF16),
                pltpu.VMEM((n, batch, 8, 128), F32),
                pltpu.SemaphoreType.DMA,
                pltpu.SemaphoreType.DMA((SLOTS,)),
                pltpu.SemaphoreType.DMA((SLOTS,)),
                pltpu.SemaphoreType.DMA((groups, n - 1)),
                pltpu.SemaphoreType.DMA((groups, n - 1)),
                pltpu.SemaphoreType.DMA((groups, n - 1)),
                pltpu.SemaphoreType.DMA((groups, n - 1)),
            ],
            compiler_params=pltpu.CompilerParams(collective_id=0, has_side_effects=True, vmem_limit_bytes=48 * 2**20),
        )(pltpu.with_memory_space_constraint(q, pltpu.HBM), k.reshape(batch, rows, head), v.reshape(batch, rows, head))

    return jax.shard_map(
        step,
        mesh=mesh,
        in_specs=(P("dp", None, None), P("dp", "sp", None, None), P("dp", "sp", None, None)),
        out_specs=P("dp", None, None),
        check_vma=False,
    )
```

```python
import functools
import math

import jax
import jax.numpy as jnp
from jax import lax
from jax.experimental import pallas as pl
from jax.experimental.pallas import tpu as pltpu
from jax.sharding import PartitionSpec as P

MESH = pl.DeviceIdType.MESH
F32, BF16 = jnp.float32, jnp.bfloat16
SLOTS = 3
LAG = 4
LEAD = 4
TILE = 256


def lane_fold(x, kind, kinds, reduce, fill):
    out = None
    for g in range(kinds):
        r = reduce(jnp.where(kind == g, x, fill), axis=1, keepdims=True)
        out = jnp.broadcast_to(r, x.shape) if out is None else jnp.where(kind == g, r, out)
    return out


def kernel(n, heads_kv, q_hbm, k_hbm, v_hbm, out_ref, qbuf, kbuf, vbuf, s0, s1, h0, h1, m0, m1, l0, l1, one_ref, mask_ref, part, stat, qsem, ksem, vsem,
           part_send, part_recv, stat_send, stat_recv):
    me = lax.axis_index("sp")
    batch, heads, head = qbuf.shape
    slots, rows = kbuf.shape[:2]
    half = rows // 2
    tiles = half // TILE
    factor = head**-0.5 * math.log2(math.e)
    groups = batch // 2 - 1

    def k_copy(i):
        slot = lax.rem(i, slots)
        return pltpu.make_async_copy(k_hbm.at[i], kbuf.at[slot], ksem.at[slot])

    def v_copy(i):
        slot = lax.rem(i, slots)
        return pltpu.make_async_copy(v_hbm.at[i], vbuf.at[slot], vsem.at[slot])

    def pieces(g, src, first, count, row):
        return (
            (part.at[src, pl.ds(first, count)], part_send, part_recv),
            (stat.at[src, row], stat_send, stat_recv),
        )

    def transfers(g, *which):
        out = []
        for off in (*range(2, n - 1), n - 1, 1):
            to = {"sp": lax.rem(me + off, n)}
            for ref, ssem, rsem in pieces(g, me, *which):
                out.append(pltpu.make_async_remote_copy(ref, ref, ssem.at[g, off - 1], rsem.at[g, off - 1], device_id=to, device_id_type=MESH))
        return out

    def arrivals(g, *which):
        out = []
        for off in range(1, n):
            src = lax.rem(me + n - off, n)
            for ref, ssem, rsem in pieces(g, src, *which):
                out.append(pltpu.make_async_remote_copy(ref, ref, ssem.at[g, off - 1], rsem.at[g, off - 1], device_id={"sp": src}, device_id_type=MESH))
        return out

    q_copy = pltpu.make_async_copy(q_hbm, qbuf, qsem)
    q_copy.start()
    k_copy(0).start()

    barrier = pltpu.get_barrier_semaphore()
    for off in range(1, n):
        pl.semaphore_signal(barrier, inc=1, device_id={"sp": lax.rem(me + off, n)}, device_id_type=MESH)

    per = heads // heads_kv
    own = lax.broadcasted_iota(jnp.int32, (heads, TILE), 0) // per == lax.rem(lax.broadcasted_iota(jnp.int32, (heads, TILE), 1), heads_kv)
    one_ref[...] = jnp.ones_like(one_ref)
    mask_ref[...] = jnp.where(own, 1.0, 0.0).astype(BF16)
    kind = lax.rem(lax.broadcasted_iota(jnp.int32, (8, TILE), 1), heads_kv)
    lane = lax.broadcasted_iota(jnp.int32, (8, 128), 1)
    low = lax.broadcasted_iota(jnp.int32, (8, 128), 0) < 4

    def scores(i, s_ref, h_ref):
        slot = lax.rem(i, slots)
        q = qbuf[i]
        zero = jnp.zeros_like(q)
        lhs = jnp.concatenate([jnp.concatenate([q, zero], 1), jnp.concatenate([zero, q], 1)], 0)
        top = None
        for c in range(tiles):
            lanes = slice(c * TILE, (c + 1) * TILE)
            rhs = jnp.concatenate([kbuf[slot, c * TILE : (c + 1) * TILE, :], kbuf[slot, half + c * TILE : half + (c + 1) * TILE, :]], 1)
            s = lax.dot_general(lhs, rhs, (((1,), (1,)), ((), ())), preferred_element_type=F32)
            for x in range(2):
                r = s[heads * x : heads * (x + 1)]
                a = jnp.where(kind == 0, r[0:8], jnp.where(kind == 1, r[16:24], jnp.where(kind == 2, r[24:32], r[40:48])))
                b = jnp.where(kind < 2, r[8:16], r[32:40])
                s_ref[x, 0:8, lanes] = a
                s_ref[x, 8:16, lanes] = b
                top = (a, b) if top is None else (jnp.maximum(top[0], a), jnp.maximum(top[1], b))
            if c % 2:
                yield
        for x in range(2):
            h_ref[x] = jnp.maximum(top[x][:, :128], top[x][:, 128:])

    def weigh(i, s_ref, h_ref, m_ref, l_ref, alone=False):
        slot = lax.rem(i, slots)
        high = [lane_fold(h_ref[x], kind[:, :128], heads_kv, jnp.max, -jnp.inf) for x in range(2)]
        for x in range(2):
            m_ref[x] = high[x]
        yield
        wide = [jnp.concatenate([h, h], 1) for h in high]
        sums = [jnp.zeros((8, TILE), F32), jnp.zeros((8, TILE), F32)]
        acc = [None, None]
        mask = mask_ref[...]
        for c in range(tiles):
            lanes = slice(c * TILE, (c + 1) * TILE)
            both = []
            for x in range(2):
                a = jnp.exp2((s_ref[x, 0:8, lanes] - wide[0]) * factor)
                b = jnp.exp2((s_ref[x, 8:16, lanes] - wide[1]) * factor)
                sums = [sums[0] + a, sums[1] + b]
                both.append(jnp.concatenate([a, b, a, a, b, a], 0).astype(BF16) * mask)
            w = jnp.concatenate(both, 0)
            rhs = jnp.concatenate([vbuf[slot, c * TILE : (c + 1) * TILE, :], vbuf[slot, half + c * TILE : half + (c + 1) * TILE, :]], 1)
            o = jnp.dot(w, rhs, preferred_element_type=F32)
            acc[c % 2] = o if acc[c % 2] is None else acc[c % 2] + o
            if c % 2:
                yield
        o = acc[0] + (acc[1] * one_ref[...] if alone else acc[1])
        part[me, i] = (o[:heads, :head] + o[heads:, head:]).astype(BF16)
        for x in range(2):
            l_ref[x] = sums[x][:, :128] + sums[x][:, 128:]

    def settle(row, odd, m_ref, l_ref):
        sums = [lane_fold(l_ref[x], kind[:, :128], heads_kv, jnp.sum, 0.0) for x in range(2)]
        spot = lane & 63
        new = jnp.where(spot < 16, m_ref[0], jnp.where(spot < 32, m_ref[1], jnp.where(spot < 48, sums[0], sums[1])))
        stat[me, row] = jnp.where(lane < 64, stat[me, row], new) if odd else new
        yield

    def run(*gens):
        gens = list(gens)
        while gens:
            for g in list(gens):
                try:
                    next(g)
                except StopIteration:
                    gens.remove(g)

    def block(first, second, *others):
        others = list(others)

        def step(g, count=1):
            for _ in range(count):
                next(g, None)

        step(second)
        step(first, LEAD)
        while True:
            for g in others:
                step(g)
            step(second, 2)
            if next(first, StopIteration) is StopIteration:
                break
        run(second, *others)

    def combine(i, row, odd):
        st = [stat[p, row] for p in range(n)]
        top = functools.reduce(jnp.maximum, st)
        scale = [jnp.exp2((s - top) * factor) for s in st]
        total = sum(w * pltpu.roll(s, 128 - 32, 1) for w, s in zip(scale, st))
        inv = 1.0 / total
        yield
        acc = None
        for p in range(n):
            w = scale[p] * inv

            def col(c):
                c = c + 64 * odd
                return jnp.broadcast_to(w[:, c : c + 1], (8, head))

            m01 = jnp.where(low, col(16), col(17))
            m23 = jnp.where(low, col(18), col(19))
            full = jnp.concatenate([col(0), m01, col(1), col(2), m23, col(3)], 0)
            term = part[p, i].astype(F32) * full
            acc = term if acc is None else acc + term
            yield
        out_ref[i] = acc.astype(BF16)

    def wait_arrivals(*which):
        for c in arrivals(*which):
            c.wait_recv()

    def send(*which):
        for c in transfers(*which):
            c.start()

    def wait_sent(*which):
        for c in transfers(*which):
            c.wait_send()

    pl.delay(150)
    k_copy(1).start()
    pl.delay(300)
    v_copy(0).start()
    pl.delay(400)
    k_copy(2).start()
    q_copy.wait()
    k_copy(0).wait()

    def second():
        for _ in range(4):
            yield
        v_copy(1).start()

    run(scores(0, s0, h0), second())
    pl.semaphore_wait(barrier, n - 1)

    def fetch(i):
        for copy, later in ((k_copy, i + slots), (v_copy, i + slots - 1)):
            @pl.when(later < batch)
            def _():
                copy(later).start()

    def pair(g):
        return g, 2 * g, 2, g

    def combine_pair(g):
        return [combine(2 * g, g, 0), combine(2 * g + 1, g, 1)]

    def body(full, j, _):
        i = 2 * j
        fetch(i)
        extra = []
        if full:
            wait_arrivals(*pair(j - LAG))
            wait_sent(*pair(j - LAG))
            extra = combine_pair(j - LAG)
        k_copy(i + 1).wait()
        v_copy(i).wait()
        block(scores(i + 1, s1, h1), weigh(i, s0, h0, m0, l0), settle(lax.max(j - 1, 0), 1, m1, l1), *extra[:1])
        fetch(i + 1)
        if full:
            send(*pair(j - 1))
        else:
            @pl.when(j >= 1)
            def _():
                send(*pair(j - 1))

        k_copy(i + 2).wait()
        v_copy(i + 1).wait()
        block(scores(i + 2, s0, h0), weigh(i + 1, s1, h1, m1, l1), settle(j, 0, m0, l0), *extra[1:])
        return 0

    lax.fori_loop(0, LAG, functools.partial(body, False), 0)
    lax.fori_loop(LAG, groups, functools.partial(body, True), 0)
    last = batch - 1
    tail = [pair(groups - 1), (groups, last - 1, 1, groups), (groups + 1, last, 1, groups + 1)]
    k_copy(last).wait()
    run(settle(groups - 1, 1, m1, l1), scores(last, s1, h1))
    send(*tail[0])
    v_copy(last - 1).wait()
    run(weigh(last - 1, s0, h0, m0, l0, True))
    run(settle(groups, 0, m0, l0))
    send(*tail[1])
    final = weigh(last, s1, h1, m1, l1, True)
    next(final)
    v_copy(last).wait()
    run(final)
    run(settle(groups + 1, 0, m1, l1))
    send(*tail[2])

    def rest(g, _):
        wait_arrivals(*pair(g))
        wait_sent(*pair(g))
        run(*combine_pair(g))
        return 0

    lax.fori_loop(groups - LAG, groups, rest, 0)
    for s in tail[1:]:
        wait_arrivals(*s)
        run(combine(s[1], s[3], 0))
    for s in tail[1:]:
        wait_sent(*s)


def solution(mesh):
    n = mesh.shape["sp"]

    def step(q, k, v):
        batch, heads, head = q.shape
        tokens, heads_kv = k.shape[1:3]
        rows = tokens * heads_kv
        groups = batch // 2 + 1
        any_spec = pl.BlockSpec(memory_space=pl.ANY)
        return pl.pallas_call(
            functools.partial(kernel, n, heads_kv),
            out_shape=pltpu.VMEM(q.shape, BF16),
            in_specs=[any_spec] * 3,
            out_specs=pl.BlockSpec(memory_space=pltpu.VMEM),
            scratch_shapes=[
                pltpu.VMEM((batch, heads, head), BF16),
                pltpu.VMEM((SLOTS, rows, head), BF16),
                pltpu.VMEM((SLOTS, rows, head), BF16),
                pltpu.VMEM((2, 16, rows // 2), F32),
                pltpu.VMEM((2, 16, rows // 2), F32),
                *[pltpu.VMEM((2, 8, 128), F32)] * 6,
                pltpu.VMEM((2 * heads, TILE), F32),
                pltpu.VMEM((heads, TILE), BF16),
                pltpu.VMEM((n, batch, heads, head), BF16),
                pltpu.VMEM((n, groups, 8, 128), F32),
                pltpu.SemaphoreType.DMA,
                pltpu.SemaphoreType.DMA((SLOTS,)),
                pltpu.SemaphoreType.DMA((SLOTS,)),
                pltpu.SemaphoreType.DMA((groups, n - 1)),
                pltpu.SemaphoreType.DMA((groups, n - 1)),
                pltpu.SemaphoreType.DMA((groups, n - 1)),
                pltpu.SemaphoreType.DMA((groups, n - 1)),
            ],
            compiler_params=pltpu.CompilerParams(collective_id=0, has_side_effects=True, vmem_limit_bytes=48 * 2**20),
        )(pltpu.with_memory_space_constraint(q, pltpu.HBM), k.reshape(batch, rows, head), v.reshape(batch, rows, head))

    return jax.shard_map(
        step,
        mesh=mesh,
        in_specs=(P("dp", None, None), P("dp", "sp", None, None), P("dp", "sp", None, None)),
        out_specs=P("dp", None, None),
        check_vma=False,
    )
```

```python
import functools
import math

import jax
import jax.numpy as jnp
from jax import lax
from jax.experimental import pallas as pl
from jax.experimental.pallas import tpu as pltpu
from jax.sharding import PartitionSpec as P

MESH = pl.DeviceIdType.MESH
F32, BF16 = jnp.float32, jnp.bfloat16
SLOTS = 3
LAG = 4
LEAD = 4
TILE = 256


def lane_fold(x, kind, kinds, reduce, fill):
    out = None
    for g in range(kinds):
        r = reduce(jnp.where(kind == g, x, fill), axis=1, keepdims=True)
        out = jnp.broadcast_to(r, x.shape) if out is None else jnp.where(kind == g, r, out)
    return out


def kernel(n, heads_kv, q_hbm, k_hbm, v_hbm, out_ref, qbuf, kbuf, vbuf, s0, s1, h0, h1, m0, m1, l0, l1, one_ref, mask_ref, part, stat, qsem, ksem, vsem,
           part_send, part_recv, stat_send, stat_recv):
    me = lax.axis_index("sp")
    batch, heads, head = qbuf.shape
    slots, rows = kbuf.shape[:2]
    half = rows // 2
    tiles = half // TILE
    factor = head**-0.5 * math.log2(math.e)
    groups = batch // 2 - 1

    def k_copy(i):
        slot = lax.rem(i, slots)
        return pltpu.make_async_copy(k_hbm.at[i], kbuf.at[slot], ksem.at[slot])

    def v_copy(i):
        slot = lax.rem(i, slots)
        return pltpu.make_async_copy(v_hbm.at[i], vbuf.at[slot], vsem.at[slot])

    def pieces(g, src, first, count, row):
        return (
            (part.at[src, pl.ds(first, count)], part_send, part_recv),
            (stat.at[src, row], stat_send, stat_recv),
        )

    def transfers(g, *which):
        out = []
        for off in (*range(2, n - 1), n - 1, 1):
            to = {"sp": lax.rem(me + off, n)}
            for ref, ssem, rsem in pieces(g, me, *which):
                out.append(pltpu.make_async_remote_copy(ref, ref, ssem.at[g, off - 1], rsem.at[g, off - 1], device_id=to, device_id_type=MESH))
        return out

    def arrivals(g, *which):
        out = []
        for off in range(1, n):
            src = lax.rem(me + n - off, n)
            for ref, ssem, rsem in pieces(g, src, *which):
                out.append(pltpu.make_async_remote_copy(ref, ref, ssem.at[g, off - 1], rsem.at[g, off - 1], device_id={"sp": src}, device_id_type=MESH))
        return out

    q_copy = pltpu.make_async_copy(q_hbm, qbuf, qsem)
    q_copy.start()
    k_copy(0).start()

    barrier = pltpu.get_barrier_semaphore()
    for off in range(1, n):
        pl.semaphore_signal(barrier, inc=1, device_id={"sp": lax.rem(me + off, n)}, device_id_type=MESH)

    per = heads // heads_kv
    own = lax.broadcasted_iota(jnp.int32, (heads, TILE), 0) // per == lax.rem(lax.broadcasted_iota(jnp.int32, (heads, TILE), 1), heads_kv)
    one_ref[...] = jnp.ones_like(one_ref)
    mask_ref[...] = jnp.where(own, 1.0, 0.0).astype(BF16)
    kind = lax.rem(lax.broadcasted_iota(jnp.int32, (8, TILE), 1), heads_kv)
    lane = lax.broadcasted_iota(jnp.int32, (8, 128), 1)
    low = lax.broadcasted_iota(jnp.int32, (8, 128), 0) < 4

    def scores(i, s_ref, h_ref):
        slot = lax.rem(i, slots)
        q = qbuf[i]
        zero = jnp.zeros_like(q)
        lhs = jnp.concatenate([jnp.concatenate([q, zero], 1), jnp.concatenate([zero, q], 1)], 0)
        top = None
        for c in range(tiles):
            lanes = slice(c * TILE, (c + 1) * TILE)
            rhs = jnp.concatenate([kbuf[slot, c * TILE : (c + 1) * TILE, :], kbuf[slot, half + c * TILE : half + (c + 1) * TILE, :]], 1)
            s = lax.dot_general(lhs, rhs, (((1,), (1,)), ((), ())), preferred_element_type=F32)
            for x in range(2):
                r = s[heads * x : heads * (x + 1)]
                a = jnp.where(kind == 0, r[0:8], jnp.where(kind == 1, r[16:24], jnp.where(kind == 2, r[24:32], r[40:48])))
                b = jnp.where(kind < 2, r[8:16], r[32:40])
                s_ref[x, 0:8, lanes] = a
                s_ref[x, 8:16, lanes] = b
                top = (a, b) if top is None else (jnp.maximum(top[0], a), jnp.maximum(top[1], b))
            if c % 2:
                yield
        for x in range(2):
            h_ref[x] = jnp.maximum(top[x][:, :128], top[x][:, 128:])

    def weigh(i, s_ref, h_ref, m_ref, l_ref, alone=False):
        slot = lax.rem(i, slots)
        high = [lane_fold(h_ref[x], kind[:, :128], heads_kv, jnp.max, -jnp.inf) for x in range(2)]
        for x in range(2):
            m_ref[x] = high[x]
        yield
        wide = [jnp.concatenate([h, h], 1) for h in high]
        sums = [jnp.zeros((8, TILE), F32), jnp.zeros((8, TILE), F32)]
        acc = [None, None]
        mask = mask_ref[...]
        for c in range(tiles):
            lanes = slice(c * TILE, (c + 1) * TILE)
            both = []
            for x in range(2):
                a = jnp.exp2((s_ref[x, 0:8, lanes] - wide[0]) * factor)
                b = jnp.exp2((s_ref[x, 8:16, lanes] - wide[1]) * factor)
                sums = [sums[0] + a, sums[1] + b]
                both.append(jnp.concatenate([a, b, a, a, b, a], 0).astype(BF16) * mask)
            w = jnp.concatenate(both, 0)
            rhs = jnp.concatenate([vbuf[slot, c * TILE : (c + 1) * TILE, :], vbuf[slot, half + c * TILE : half + (c + 1) * TILE, :]], 1)
            o = jnp.dot(w, rhs, preferred_element_type=F32)
            acc[c % 2] = o if acc[c % 2] is None else acc[c % 2] + o
            if c % 2:
                yield
        o = acc[0] + (acc[1] * one_ref[...] if alone else acc[1])
        part[me, i] = (o[:heads, :head] + o[heads:, head:]).astype(BF16)
        for x in range(2):
            l_ref[x] = sums[x][:, :128] + sums[x][:, 128:]

    def settle(row, odd, m_ref, l_ref):
        sums = [lane_fold(l_ref[x], kind[:, :128], heads_kv, jnp.sum, 0.0) for x in range(2)]
        spot = lane & 63
        new = jnp.where(spot < 16, m_ref[0], jnp.where(spot < 32, m_ref[1], jnp.where(spot < 48, sums[0], sums[1])))
        stat[me, row] = jnp.where(lane < 64, stat[me, row], new) if odd else new
        yield

    def run(*gens):
        gens = list(gens)
        while gens:
            for g in list(gens):
                try:
                    next(g)
                except StopIteration:
                    gens.remove(g)

    def block(first, second, *others):
        others = list(others)

        def step(g, count=1):
            for _ in range(count):
                next(g, None)

        step(second)
        step(first, LEAD)
        while True:
            for g in others:
                step(g)
            step(second, 2)
            if next(first, StopIteration) is StopIteration:
                break
        run(second, *others)

    def combine(i, row, odd):
        st = [stat[p, row] for p in range(n)]
        top = functools.reduce(jnp.maximum, st)
        scale = [jnp.exp2((s - top) * factor) for s in st]
        total = sum(w * pltpu.roll(s, 128 - 32, 1) for w, s in zip(scale, st))
        inv = 1.0 / total
        yield
        acc = None
        for p in range(n):
            w = scale[p] * inv

            def col(c):
                c = c + 64 * odd
                return jnp.broadcast_to(w[:, c : c + 1], (8, head))

            m01 = jnp.where(low, col(16), col(17))
            m23 = jnp.where(low, col(18), col(19))
            full = jnp.concatenate([col(0), m01, col(1), col(2), m23, col(3)], 0)
            term = part[p, i].astype(F32) * full
            acc = term if acc is None else acc + term
            yield
        out_ref[i] = acc.astype(BF16)

    def wait_arrivals(*which):
        for c in arrivals(*which):
            c.wait_recv()

    def send(*which):
        for c in transfers(*which):
            c.start()

    def wait_sent(*which):
        for c in transfers(*which):
            c.wait_send()

    pl.delay(250)
    k_copy(1).start()
    pl.delay(500)
    v_copy(0).start()
    pl.delay(600)
    k_copy(2).start()
    q_copy.wait()
    k_copy(0).wait()

    def second():
        for _ in range(3):
            yield
        v_copy(1).start()

    run(scores(0, s0, h0), second())
    pl.semaphore_wait(barrier, n - 1)

    def fetch(i):
        for copy, later in ((k_copy, i + slots), (v_copy, i + slots - 1)):
            @pl.when(later < batch)
            def _():
                copy(later).start()

    def pair(g):
        return g, 2 * g, 2, g

    def combine_pair(g):
        return [combine(2 * g, g, 0), combine(2 * g + 1, g, 1)]

    def body(full, j, _):
        i = 2 * j
        fetch(i)
        extra = []
        if full:
            wait_arrivals(*pair(j - LAG))
            wait_sent(*pair(j - LAG))
            extra = combine_pair(j - LAG)
        k_copy(i + 1).wait()
        v_copy(i).wait()
        block(scores(i + 1, s1, h1), weigh(i, s0, h0, m0, l0), settle(lax.max(j - 1, 0), 1, m1, l1), *extra[:1])
        fetch(i + 1)
        if full:
            send(*pair(j - 1))
        else:
            @pl.when(j >= 1)
            def _():
                send(*pair(j - 1))

        k_copy(i + 2).wait()
        v_copy(i + 1).wait()
        block(scores(i + 2, s0, h0), weigh(i + 1, s1, h1, m1, l1), settle(j, 0, m0, l0), *extra[1:])
        return 0

    lax.fori_loop(0, LAG, functools.partial(body, False), 0)
    lax.fori_loop(LAG, groups, functools.partial(body, True), 0)
    last = batch - 1
    tail = [pair(groups - 1), (groups, last - 1, 1, groups), (groups + 1, last, 1, groups + 1)]
    run(settle(groups - 1, 1, m1, l1))
    send(*tail[0])
    k_copy(last).wait()
    v_copy(last - 1).wait()
    block(scores(last, s1, h1), weigh(last - 1, s0, h0, m0, l0))
    final = weigh(last, s1, h1, m1, l1, True)
    next(final)
    run(settle(groups, 0, m0, l0))
    send(*tail[1])
    v_copy(last).wait()
    run(final)
    run(settle(groups + 1, 0, m1, l1))
    send(*tail[2])

    def rest(g, _):
        wait_arrivals(*pair(g))
        wait_sent(*pair(g))
        run(*combine_pair(g))
        return 0

    lax.fori_loop(groups - LAG, groups, rest, 0)
    for s in tail[1:]:
        wait_arrivals(*s)
        run(combine(s[1], s[3], 0))
    for s in tail[1:]:
        wait_sent(*s)


def solution(mesh):
    n = mesh.shape["sp"]

    def step(q, k, v):
        batch, heads, head = q.shape
        tokens, heads_kv = k.shape[1:3]
        rows = tokens * heads_kv
        groups = batch // 2 + 1
        any_spec = pl.BlockSpec(memory_space=pl.ANY)
        return pl.pallas_call(
            functools.partial(kernel, n, heads_kv),
            out_shape=pltpu.VMEM(q.shape, BF16),
            in_specs=[any_spec] * 3,
            out_specs=pl.BlockSpec(memory_space=pltpu.VMEM),
            scratch_shapes=[
                pltpu.VMEM((batch, heads, head), BF16),
                pltpu.VMEM((SLOTS, rows, head), BF16),
                pltpu.VMEM((SLOTS, rows, head), BF16),
                pltpu.VMEM((2, 16, rows // 2), F32),
                pltpu.VMEM((2, 16, rows // 2), F32),
                *[pltpu.VMEM((2, 8, 128), F32)] * 6,
                pltpu.VMEM((2 * heads, TILE), F32),
                pltpu.VMEM((heads, TILE), BF16),
                pltpu.VMEM((n, batch, heads, head), BF16),
                pltpu.VMEM((n, groups, 8, 128), F32),
                pltpu.SemaphoreType.DMA,
                pltpu.SemaphoreType.DMA((SLOTS,)),
                pltpu.SemaphoreType.DMA((SLOTS,)),
                pltpu.SemaphoreType.DMA((groups, n - 1)),
                pltpu.SemaphoreType.DMA((groups, n - 1)),
                pltpu.SemaphoreType.DMA((groups, n - 1)),
                pltpu.SemaphoreType.DMA((groups, n - 1)),
            ],
            compiler_params=pltpu.CompilerParams(collective_id=0, has_side_effects=True, vmem_limit_bytes=48 * 2**20),
        )(pltpu.with_memory_space_constraint(q, pltpu.HBM), k.reshape(batch, rows, head), v.reshape(batch, rows, head))

    return jax.shard_map(
        step,
        mesh=mesh,
        in_specs=(P("dp", None, None), P("dp", "sp", None, None), P("dp", "sp", None, None)),
        out_specs=P("dp", None, None),
        check_vma=False,
    )
```

```python
import functools
import math

import jax
import jax.numpy as jnp
from jax import lax
from jax.experimental import pallas as pl
from jax.experimental.pallas import tpu as pltpu
from jax.sharding import PartitionSpec as P

MESH = pl.DeviceIdType.MESH
F32, BF16 = jnp.float32, jnp.bfloat16
SLOTS = 3
LAG = 4
LEAD = 4
SENDS, ARRIVALS = 8, 9
TILE = 256


def lane_fold(x, kind, kinds, reduce, fill):
    out = None
    for g in range(kinds):
        r = reduce(jnp.where(kind == g, x, fill), axis=1, keepdims=True)
        out = jnp.broadcast_to(r, x.shape) if out is None else jnp.where(kind == g, r, out)
    return out


def kernel(n, heads_kv, q_hbm, k_hbm, v_hbm, out_ref, qbuf, kbuf, vbuf, s0, s1, h0, h1, m0, m1, l0, l1, one_ref, mask_ref, part, stat, qsem, ksem, vsem,
           part_send, part_recv, stat_send, stat_recv):
    me = lax.axis_index("sp")
    batch, heads, head = qbuf.shape
    slots, rows = kbuf.shape[:2]
    half = rows // 2
    tiles = half // TILE
    factor = head**-0.5 * math.log2(math.e)
    groups = batch // 2 - 1

    def k_copy(i):
        slot = lax.rem(i, slots)
        return pltpu.make_async_copy(k_hbm.at[i], kbuf.at[slot], ksem.at[slot])

    def v_copy(i):
        slot = lax.rem(i, slots)
        return pltpu.make_async_copy(v_hbm.at[i], vbuf.at[slot], vsem.at[slot])

    def turn(g, ring):
        return g % ring if isinstance(g, int) else lax.rem(g, ring)

    def pieces(g, src, first, count, row):
        return (
            (part.at[src, pl.ds(first, count)], part_send, part_recv),
            (stat.at[src, row], stat_send, stat_recv),
        )

    def transfers(g, *which):
        out = []
        for off in (*range(2, n - 1), n - 1, 1):
            to = {"sp": lax.rem(me + off, n)}
            for ref, ssem, rsem in pieces(g, me, *which):
                out.append(pltpu.make_async_remote_copy(ref, ref, ssem.at[turn(g, SENDS), off - 1], rsem.at[turn(g, ARRIVALS), off - 1], device_id=to, device_id_type=MESH))
        return out

    def arrivals(g, *which):
        out = []
        for off in range(1, n):
            src = lax.rem(me + n - off, n)
            for ref, ssem, rsem in pieces(g, src, *which):
                out.append(pltpu.make_async_remote_copy(ref, ref, ssem.at[turn(g, SENDS), off - 1], rsem.at[turn(g, ARRIVALS), off - 1], device_id={"sp": src}, device_id_type=MESH))
        return out

    q_copy = pltpu.make_async_copy(q_hbm, qbuf, qsem)
    q_copy.start()
    k_copy(0).start()

    barrier = pltpu.get_barrier_semaphore()
    for off in range(1, n):
        pl.semaphore_signal(barrier, inc=1, device_id={"sp": lax.rem(me + off, n)}, device_id_type=MESH)

    per = heads // heads_kv
    own = lax.broadcasted_iota(jnp.int32, (heads, TILE), 0) // per == lax.rem(lax.broadcasted_iota(jnp.int32, (heads, TILE), 1), heads_kv)
    one_ref[...] = jnp.ones_like(one_ref)
    mask_ref[...] = jnp.where(own, 1.0, 0.0).astype(BF16)
    kind = lax.rem(lax.broadcasted_iota(jnp.int32, (8, TILE), 1), heads_kv)
    lane = lax.broadcasted_iota(jnp.int32, (8, 128), 1)
    low = lax.broadcasted_iota(jnp.int32, (8, 128), 0) < 4

    def scores(i, s_ref, h_ref):
        slot = lax.rem(i, slots)
        q = qbuf[i]
        zero = jnp.zeros_like(q)
        lhs = jnp.concatenate([jnp.concatenate([q, zero], 1), jnp.concatenate([zero, q], 1)], 0)
        top = None
        for c in range(tiles):
            lanes = slice(c * TILE, (c + 1) * TILE)
            rhs = jnp.concatenate([kbuf[slot, c * TILE : (c + 1) * TILE, :], kbuf[slot, half + c * TILE : half + (c + 1) * TILE, :]], 1)
            s = lax.dot_general(lhs, rhs, (((1,), (1,)), ((), ())), preferred_element_type=F32)
            for x in range(2):
                r = s[heads * x : heads * (x + 1)]
                a = jnp.where(kind == 0, r[0:8], jnp.where(kind == 1, r[16:24], jnp.where(kind == 2, r[24:32], r[40:48])))
                b = jnp.where(kind < 2, r[8:16], r[32:40])
                s_ref[x, 0:8, lanes] = a
                s_ref[x, 8:16, lanes] = b
                top = (a, b) if top is None else (jnp.maximum(top[0], a), jnp.maximum(top[1], b))
            if c % 2:
                yield
        for x in range(2):
            h_ref[x] = jnp.maximum(top[x][:, :128], top[x][:, 128:])

    def weigh(i, s_ref, h_ref, m_ref, l_ref, alone=False):
        slot = lax.rem(i, slots)
        high = [lane_fold(h_ref[x], kind[:, :128], heads_kv, jnp.max, -jnp.inf) for x in range(2)]
        for x in range(2):
            m_ref[x] = high[x]
        yield
        wide = [jnp.concatenate([h, h], 1) for h in high]
        sums = [jnp.zeros((8, TILE), F32), jnp.zeros((8, TILE), F32)]
        acc = [None, None]
        mask = mask_ref[...]
        for c in range(tiles):
            lanes = slice(c * TILE, (c + 1) * TILE)
            both = []
            for x in range(2):
                a = jnp.exp2((s_ref[x, 0:8, lanes] - wide[0]) * factor)
                b = jnp.exp2((s_ref[x, 8:16, lanes] - wide[1]) * factor)
                sums = [sums[0] + a, sums[1] + b]
                both.append(jnp.concatenate([a, b, a, a, b, a], 0).astype(BF16) * mask)
            w = jnp.concatenate(both, 0)
            rhs = jnp.concatenate([vbuf[slot, c * TILE : (c + 1) * TILE, :], vbuf[slot, half + c * TILE : half + (c + 1) * TILE, :]], 1)
            o = jnp.dot(w, rhs, preferred_element_type=F32)
            acc[c % 2] = o if acc[c % 2] is None else acc[c % 2] + o
            if c % 2:
                yield
        o = acc[0] + (acc[1] * one_ref[...] if alone else acc[1])
        part[me, i] = (o[:heads, :head] + o[heads:, head:]).astype(BF16)
        for x in range(2):
            l_ref[x] = sums[x][:, :128] + sums[x][:, 128:]

    def settle(row, odd, m_ref, l_ref):
        sums = [lane_fold(l_ref[x], kind[:, :128], heads_kv, jnp.sum, 0.0) for x in range(2)]
        spot = lane & 63
        new = jnp.where(spot < 16, m_ref[0], jnp.where(spot < 32, m_ref[1], jnp.where(spot < 48, sums[0], sums[1])))
        stat[me, row] = jnp.where(lane < 64, stat[me, row], new) if odd else new
        yield

    def run(*gens):
        gens = list(gens)
        while gens:
            for g in list(gens):
                try:
                    next(g)
                except StopIteration:
                    gens.remove(g)

    def block(first, second, *others):
        others = list(others)

        def step(g, count=1):
            for _ in range(count):
                next(g, None)

        step(second)
        step(first, LEAD)
        while True:
            for g in others:
                step(g)
            step(second, 2)
            if next(first, StopIteration) is StopIteration:
                break
        run(second, *others)

    def combine(i, row, odd):
        st = [stat[p, row] for p in range(n)]
        top = functools.reduce(jnp.maximum, st)
        scale = [jnp.exp2((s - top) * factor) for s in st]
        total = sum(w * pltpu.roll(s, 128 - 32, 1) for w, s in zip(scale, st))
        inv = 1.0 / total
        yield
        acc = None
        for p in range(n):
            w = scale[p] * inv

            def col(c):
                c = c + 64 * odd
                return jnp.broadcast_to(w[:, c : c + 1], (8, head))

            m01 = jnp.where(low, col(16), col(17))
            m23 = jnp.where(low, col(18), col(19))
            full = jnp.concatenate([col(0), m01, col(1), col(2), m23, col(3)], 0)
            term = part[p, i].astype(F32) * full
            acc = term if acc is None else acc + term
            yield
        out_ref[i] = acc.astype(BF16)

    def wait_arrivals(*which):
        for c in arrivals(*which):
            c.wait_recv()

    def send(*which):
        for c in transfers(*which):
            c.start()

    def wait_sent(*which):
        for c in transfers(*which):
            c.wait_send()

    pl.delay(250)
    k_copy(1).start()
    pl.delay(500)
    v_copy(0).start()
    pl.delay(600)
    k_copy(2).start()
    q_copy.wait()
    k_copy(0).wait()

    def second():
        for _ in range(3):
            yield
        v_copy(1).start()

    run(scores(0, s0, h0), second())
    pl.semaphore_wait(barrier, n - 1)

    def fetch(i):
        for copy, later in ((k_copy, i + slots), (v_copy, i + slots - 1)):
            @pl.when(later < batch)
            def _():
                copy(later).start()

    def pair(g):
        return g, 2 * g, 2, g

    def combine_pair(g):
        return [combine(2 * g, g, 0), combine(2 * g + 1, g, 1)]

    def body(full, j, _):
        i = 2 * j
        fetch(i)
        extra = []
        if full:
            wait_arrivals(*pair(j - LAG))
            wait_sent(*pair(j - LAG))
            extra = combine_pair(j - LAG)
        k_copy(i + 1).wait()
        v_copy(i).wait()
        block(scores(i + 1, s1, h1), weigh(i, s0, h0, m0, l0), settle(lax.max(j - 1, 0), 1, m1, l1), *extra[:1])
        fetch(i + 1)
        if full:
            send(*pair(j - 1))
        else:
            @pl.when(j >= 1)
            def _():
                send(*pair(j - 1))

        k_copy(i + 2).wait()
        v_copy(i + 1).wait()
        block(scores(i + 2, s0, h0), weigh(i + 1, s1, h1, m1, l1), settle(j, 0, m0, l0), *extra[1:])
        return 0

    lax.fori_loop(0, LAG, functools.partial(body, False), 0)
    lax.fori_loop(LAG, groups, functools.partial(body, True), 0)
    last = batch - 1
    tail = [pair(groups - 1), (groups, last - 1, 1, groups), (groups + 1, last, 1, groups + 1)]
    run(settle(groups - 1, 1, m1, l1))
    send(*tail[0])
    k_copy(last).wait()
    v_copy(last - 1).wait()
    block(scores(last, s1, h1), weigh(last - 1, s0, h0, m0, l0))
    final = weigh(last, s1, h1, m1, l1, True)
    next(final)
    run(settle(groups, 0, m0, l0))
    send(*tail[1])
    v_copy(last).wait()
    run(final)
    run(settle(groups + 1, 0, m1, l1))
    send(*tail[2])

    def rest(g, _):
        wait_arrivals(*pair(g))
        wait_sent(*pair(g))
        run(*combine_pair(g))
        return 0

    lax.fori_loop(groups - LAG, groups, rest, 0)
    for s in tail[1:]:
        wait_arrivals(*s)
        run(combine(s[1], s[3], 0))
    for s in tail[1:]:
        wait_sent(*s)


def solution(mesh):
    n = mesh.shape["sp"]

    def step(q, k, v):
        batch, heads, head = q.shape
        tokens, heads_kv = k.shape[1:3]
        rows = tokens * heads_kv
        groups = batch // 2 + 1
        any_spec = pl.BlockSpec(memory_space=pl.ANY)
        return pl.pallas_call(
            functools.partial(kernel, n, heads_kv),
            out_shape=pltpu.VMEM(q.shape, BF16),
            in_specs=[any_spec] * 3,
            out_specs=pl.BlockSpec(memory_space=pltpu.VMEM),
            scratch_shapes=[
                pltpu.VMEM((batch, heads, head), BF16),
                pltpu.VMEM((SLOTS, rows, head), BF16),
                pltpu.VMEM((SLOTS, rows, head), BF16),
                pltpu.VMEM((2, 16, rows // 2), F32),
                pltpu.VMEM((2, 16, rows // 2), F32),
                *[pltpu.VMEM((2, 8, 128), F32)] * 6,
                pltpu.VMEM((2 * heads, TILE), F32),
                pltpu.VMEM((heads, TILE), BF16),
                pltpu.VMEM((n, batch, heads, head), BF16),
                pltpu.VMEM((n, groups, 8, 128), F32),
                pltpu.SemaphoreType.DMA,
                pltpu.SemaphoreType.DMA((SLOTS,)),
                pltpu.SemaphoreType.DMA((SLOTS,)),
                pltpu.SemaphoreType.DMA((SENDS, n - 1)),
                pltpu.SemaphoreType.DMA((ARRIVALS, n - 1)),
                pltpu.SemaphoreType.DMA((SENDS, n - 1)),
                pltpu.SemaphoreType.DMA((ARRIVALS, n - 1)),
            ],
            compiler_params=pltpu.CompilerParams(collective_id=0, has_side_effects=True, vmem_limit_bytes=48 * 2**20),
        )(pltpu.with_memory_space_constraint(q, pltpu.HBM), k.reshape(batch, rows, head), v.reshape(batch, rows, head))

    return jax.shard_map(
        step,
        mesh=mesh,
        in_specs=(P("dp", None, None), P("dp", "sp", None, None), P("dp", "sp", None, None)),
        out_specs=P("dp", None, None),
        check_vma=False,
    )
```
